512 devices in a mesh: owner: 32 (over y, x), rows: 16 (over z, core).
Axes of the slice: x: 4, y: 8, z: 8, core: 2. Of those that a mesh axis runs over, the one named last changes fastest.
Arguments:
- w_down: float32 [64, 1408, 2048], P('owner', None, 'rows'), may hold values from -0.21875 to 0.21875
- router_weight: float32 [2048, 64], P('rows', 'owner'), may hold values from -0.125 to 0.125
- router_gain: float32 [2048], P('rows'), may hold values from 0.25 to 1.75
Outputs:
- serve_down: bfloat16 [64, 1408, 2048], P('owner')
- scale_down: float32 [64, 1408], P('owner')
- serve_router: bfloat16 [2048, 64], replicated
The draws below stay inside these ranges and needn't reach their ends.
All inputs are finite; a program needn't handle non-finite values. Where the reference program divides by a largest or mean magnitude, that divisor is 1e-20 or more.
Results may differ from the reference program's by a relative error of at most 0.001.
Values may be sent and summed in bfloat16 or wider, within the bound.
A program may use at most 128 MiB of HBM per device.

```python
import jax
import jax.numpy as jnp

EXPERTS = 64
D_MODEL = 2048
D_EXPERT = 1408


def raised(result, stream_key, source, target, parts, factor):
    owner, partner = [(jnp.arange(result.shape[dim]) // (result.shape[dim] // parts)).reshape([-1 if axis == dim else 1 for axis in range(result.ndim)]) for dim in (source, target)]
    chosen = jax.random.permutation(stream_key, parts)[partner]
    strong = (owner == chosen) | (owner == (partner + parts // 2) % parts)
    return jnp.where(strong, factor * result, result)


def levels(own_key, shape, split, low, high):
    gain = 1.0
    for axis_at, parts in split:
        draws = jax.random.uniform(jax.random.fold_in(jax.random.fold_in(own_key, 6), axis_at), (parts,), jnp.float32, low / len(split), high / len(split))
        gain = gain * jnp.repeat(jnp.exp(draws), shape[axis_at] // parts).reshape((-1,) + (1,) * (len(shape) - 1 - axis_at))
    return gain


def gaussian(rng, extent, deviation, reach, cuts=(), held_as=jnp.bfloat16):
    factor_of = levels(rng, extent, cuts, -0.22, 0.18) if cuts else 1.0
    drawn = jax.random.normal(rng, extent, jnp.float32) * deviation * factor_of
    return jnp.minimum(jnp.maximum(drawn, -reach), reach).astype(held_as)


def gaussian_with(own_key, extent, scale, limit, pieces, heavy, held_as=jnp.bfloat16):
    entries = scale * jax.random.normal(own_key, extent, jnp.float32)
    if pieces:
        entries = entries * levels(own_key, extent, pieces, -0.22, 0.18)
    return jnp.clip(raised(entries, jax.random.fold_in(own_key, 3), *heavy), -limit, limit).astype(held_as)


def setup_inputs(seed: int = 0) -> dict:
    seeds = jax.random.split(jax.random.key(seed), 4)
    return {
        "w_down": gaussian_with(seeds[0], (EXPERTS, D_EXPERT, D_MODEL), D_EXPERT ** -0.5, 0.21875, ((0, 32), (2, 16)), (2, 1, 16, 2.0), jnp.float32),
        "router_weight": gaussian(seeds[1], (D_MODEL, EXPERTS), D_MODEL ** -0.5, 0.125, ((0, 16), (1, 32)), jnp.float32),
        "router_gain": jnp.clip(1.0 + 0.15 * jax.random.normal(seeds[2], (D_MODEL,), jnp.float32), 0.25, 1.75),
    }


def reference(w_down, router_weight, router_gain):
    scale_down = jnp.max(jnp.abs(w_down), axis=2)
    serve_down = (w_down / jnp.expand_dims(scale_down, 2)).astype(jnp.bfloat16)
    serve_router = (router_weight * router_gain[:, None]).astype(jnp.bfloat16)
    return serve_down, scale_down, serve_router
```

```python
import functools

import jax
import jax.numpy as jnp
from jax import lax
from jax.experimental import pallas as pl
from jax.experimental.pallas import tpu as pltpu
from jax.sharding import PartitionSpec as P

MESH = pl.DeviceIdType.MESH
BF16 = jnp.bfloat16
F32 = jnp.float32

E = 2
ROWS = 1408
LANES = 128
Z = 8
NR = 16
X, Y = 4, 8
BLOCKS = ROWS // LANES
KE = 4
K = E * KE
CH = ROWS // KE
HALF = K // 2
STEPS = 3 * K + HALF


def kernel(w_hbm, rw_hbm, gain_hbm, out, scale_out, router_out,
           w, rw, gain, mx, inv, rb,
           in_sem, mx_send, mx_recv, ring_send, right_recv, left_recv,
           die_send, die_recv, own_recv,
           r1_send, r1_recv, rx_send, rx_recv, ry_send, ry_recv):
    owner = lax.axis_index("owner")
    rows = lax.axis_index("rows")
    z, core = rows // 2, rows % 2
    x, y = owner % X, owner // X
    barrier = pltpu.get_barrier_semaphore()

    def at_rows(r):
        return {"rows": r}

    column = [(rows + d) % NR for d in range(1, NR)]
    across_x = [y * X + (x + d) % X for d in range(1, X)]
    across_y = [((y + d) % Y) * X + x for d in range(1, Y)]
    right = ((z + 1) % Z) * 2 + core
    left = ((z + Z - 1) % Z) * 2 + core
    partner = z * 2 + 1 - core

    loads = [pltpu.make_async_copy(w_hbm.at[e], w.at[e], in_sem.at[e]) for e in range(E)]
    loads.append(pltpu.make_async_copy(rw_hbm, rw, in_sem.at[E]))
    loads.append(pltpu.make_async_copy(gain_hbm, gain, in_sem.at[E + 1]))
    for load in loads:
        load.start()
    for r in column:
        pl.semaphore_signal(barrier, inc=1, device_id=at_rows(r), device_id_type=MESH)
    for o in across_x + across_y:
        pl.semaphore_signal(barrier, inc=1, device_id={"owner": o}, device_id_type=MESH)

    def maxima(e):
        loads[e].wait()
        for b in range(BLOCKS):
            block = jnp.abs(w[e, b * LANES:(b + 1) * LANES, :])
            mx[rows, e, b:b + 1, :] = jnp.max(block.T, axis=0, keepdims=True)

    def mx_copies(e):
        return [
            pltpu.make_async_remote_copy(
                src_ref=mx.at[rows, e], dst_ref=mx.at[rows, e],
                send_sem=mx_send.at[e, i], recv_sem=mx_recv.at[e, rows],
                device_id=at_rows(r), device_id_type=MESH)
            for i, r in enumerate(column)
        ]

    maxima(0)
    pl.semaphore_wait(barrier, len(column) + len(across_x) + len(across_y))
    sent = [mx_copies(e) for e in range(E)]
    for copy in sent[0]:
        copy.start()
    r1 = [
        pltpu.make_async_remote_copy(
            src_ref=rb.at[owner, rows], dst_ref=rb.at[owner, rows],
            send_sem=r1_send.at[i], recv_sem=r1_recv.at[rows],
            device_id=at_rows(r), device_id_type=MESH)
        for i, r in enumerate(column)
    ]
    maxima(1)
    for copy in sent[1]:
        copy.start()
    loads[E].wait()
    loads[E + 1].wait()
    rb[owner, rows] = (rw[...] * gain[...]).astype(BF16)
    for copy in r1:
        copy.start()

    def mx_wait(e):
        for r in column:
            pltpu.make_async_copy(mx.at[r, e], mx.at[r, e], mx_recv.at[e, r]).wait()

    def cells(origin, k):
        e, part = k // KE, k % KE
        first = pl.multiple_of(part * CH, CH)
        lanes = pl.multiple_of(origin * LANES, LANES)
        return out.at[e, pl.ds(first, CH), pl.ds(lanes, LANES)]

    def ring(to, origin, k, send, recv):
        part = cells(origin, k)
        return pltpu.make_async_remote_copy(
            src_ref=part, dst_ref=part, send_sem=send, recv_sem=recv,
            device_id=at_rows(to), device_id_type=MESH)

    def die(origin, k, send, recv):
        return ring(partner, origin, k, send, recv)

    for e in range(E):
        mx_wait(e)
        scale = jnp.max(mx[:, e], axis=0)
        inv[e] = 1.0 / scale
        for b in range(BLOCKS):
            scale_out[e:e + 1, b * LANES:(b + 1) * LANES] = scale[b:b + 1]
        done = 0
        for part in range(KE):
            need = -(-(part + 1) * CH // LANES)
            for b in range(done, need):
                factor = jnp.broadcast_to(inv[e, b:b + 1, :], (LANES, LANES)).T
                block = w[e, b * LANES:(b + 1) * LANES, :] * factor
                out[e, b * LANES:(b + 1) * LANES, pl.ds(pl.multiple_of(rows * LANES, LANES), LANES)] = block.astype(BF16)
            done = need
            k = e * KE + part
            ring(right, rows, k, ring_send.at[0, k], right_recv.at[k]).start()
            ring(left, rows, k, ring_send.at[1, k], left_recv.at[k]).start()
            die(rows, k, die_send.at[0, k], own_recv.at[k]).start()

    def step(j, _):
        d, k = j // K, j % K
        for side, (to, recv, sign) in enumerate(((right, right_recv, Z - 1), (left, left_recv, 1))):
            origin = ((z + sign * (d + 1)) % Z) * 2 + core
            far = k if side == 0 else HALF + k
            kk = jnp.where(d == 3, far, k)
            part = ring(to, origin, kk, ring_send.at[side, j], recv.at[j])
            part.wait_recv()

            @pl.when(d < 2)
            def _():
                ring(to, origin, k, ring_send.at[side, K + j], recv.at[K + j]).start()

            far_here = k - side * HALF

            @pl.when((d == 2) & (far_here >= 0) & (far_here < HALF))
            def _():
                ring(to, origin, k, ring_send.at[side, 3 * K + far_here], recv.at[3 * K + far_here]).start()

            die(origin, kk, die_send.at[1 + side, j], die_recv.at[side, j]).start()
        return 0

    def run(a, b):
        lax.fori_loop(a, b, step, 0)

    run(0, K)
    for r in column:
        pltpu.make_async_copy(rb.at[owner, r], rb.at[owner, r], r1_recv.at[r]).wait()
    rx = [
        pltpu.make_async_remote_copy(
            src_ref=rb.at[owner], dst_ref=rb.at[owner],
            send_sem=rx_send.at[i], recv_sem=rx_recv.at[x],
            device_id={"owner": o}, device_id_type=MESH)
        for i, o in enumerate(across_x)
    ]
    for copy in rx:
        copy.start()
    run(K, K + HALF)
    for i, o in enumerate(across_x):
        pltpu.make_async_copy(rb.at[o], rb.at[o], rx_recv.at[o % X]).wait()
    mine = rb.at[pl.ds(y * X, X)]
    ry = [
        pltpu.make_async_remote_copy(
            src_ref=mine, dst_ref=mine,
            send_sem=ry_send.at[i], recv_sem=ry_recv.at[y],
            device_id={"owner": o}, device_id_type=MESH)
        for i, o in enumerate(across_y)
    ]
    for copy in ry:
        copy.start()
    run(K + HALF, 2 * K)
    for o in across_y:
        theirs = rb.at[pl.ds((o // X) * X, X)]
        pltpu.make_async_copy(theirs, theirs, ry_recv.at[o // X]).wait()
    for o in range(X * Y):
        for r in range(NR):
            router_out[2 * o:2 * o + 2, r * LANES:(r + 1) * LANES] = rb[o, r]
    run(2 * K, STEPS)

    for k in range(K):
        die(partner, k, die_send.at[0, k], own_recv.at[k]).wait_recv()
        die(rows, k, die_send.at[0, k], own_recv.at[k]).wait_send()

    def last(j, _):
        d, k = j // K, j % K
        for side, sign in enumerate((Z - 1, 1)):
            theirs = ((z + sign * (d + 1)) % Z) * 2 + 1 - core
            kk = jnp.where(d == 3, HALF * side + k, k)
            there = die(theirs, kk, die_send.at[1 + side, j], die_recv.at[side, j])
            there.wait_recv()
            there.wait_send()
            ring(right, theirs, kk, ring_send.at[side, j], right_recv.at[j]).wait_send()
        return 0

    lax.fori_loop(0, STEPS, last, 0)
    for e in range(E):
        for copy in sent[e]:
            copy.wait_send()
    for copy in r1 + rx + ry:
        copy.wait_send()


def on_device(w_down, router_weight, router_gain):
    dma = pltpu.SemaphoreType.DMA
    out, scale, router = pl.pallas_call(
        kernel,
        name="serve",
        out_shape=(
            jax.ShapeDtypeStruct((E, ROWS, NR * LANES), BF16),
            jax.ShapeDtypeStruct((E, ROWS), F32),
            jax.ShapeDtypeStruct((E * X * Y, NR * LANES), BF16),
        ),
        in_specs=[pl.BlockSpec(memory_space=pltpu.HBM)] * 3,
        out_specs=(
            pl.BlockSpec(memory_space=pltpu.VMEM),
            pl.BlockSpec(memory_space=pltpu.VMEM),
            pl.BlockSpec(memory_space=pltpu.VMEM),
        ),
        scratch_shapes=[
            pltpu.VMEM((E, ROWS, LANES), F32),
            pltpu.VMEM((2, LANES), F32),
            pltpu.VMEM((1, LANES), F32),
            pltpu.VMEM((NR, E, BLOCKS, LANES), F32),
            pltpu.VMEM((E, BLOCKS, LANES), F32),
            pltpu.VMEM((X * Y, NR, 2, LANES), BF16),
            dma((E + 2,)), dma((E, NR - 1)), dma((E, NR)),
            dma((2, STEPS)), dma((STEPS,)), dma((STEPS,)),
            dma((3, STEPS)), dma((2, STEPS)), dma((K,)),
            dma((NR - 1,)), dma((NR,)), dma((X - 1,)), dma((X,)), dma((Y - 1,)), dma((Y,)),
        ],
        compiler_params=pltpu.CompilerParams(
            collective_id=0, has_side_effects=True, vmem_limit_bytes=24 * 1024 * 1024
        ),
    )(*(pltpu.with_memory_space_constraint(a, pltpu.HBM) for a in (w_down, router_weight.T, router_gain[None, :])))
    return out, scale, router.T


def solution(mesh):
    placed = (P("owner", None, "rows"), P("rows", "owner"), P("rows"))
    return jax.shard_map(
        on_device,
        mesh=mesh,
        in_specs=placed,
        out_specs=(P("owner", None, None), P("owner", None), P()),
        check_vma=False,
    )
```

```python
import jax
import jax.numpy as jnp
from jax import lax
from jax.experimental import pallas as pl
from jax.experimental.pallas import tpu as pltpu
from jax.sharding import PartitionSpec as P

MESH = pl.DeviceIdType.MESH
BF16 = jnp.bfloat16
F32 = jnp.float32

E = 2
ROWS = 1408
LANES = 128
Z = 8
NR = 16
X, Y = 4, 8
PIECES = ((0, 0, 3), (0, 3, 8), (1, 0, 11))
CHUNKS = ((0, 0, 3, 0), (0, 3, 8, 1), (1, 0, 8, 2), (1, 8, 3, 2))
K = len(CHUNKS)
ARRIVALS = tuple(
    tuple((d, k) for d in range(3) for k in range(K)) + tuple((3, k) for k in far)
    for far in ((1, 0), (2, 3))
)
STEPS = len(ARRIVALS[0])


def kernel(w_hbm, rw_hbm, gain_hbm, out, scale_out, router_out,
           w, rw, gain, mx0, mx1, mx2, mine, rb,
           in_sem, go, mx_send, mx_recv, ring_send, right_recv, left_recv,
           die_send, die_recv, own_send, own_recv,
           r1_send, r1_recv, rx_send, rx_recv, ry_send, ry_recv, rd_send, rd_recv):
    owner = lax.axis_index("owner")
    rows = lax.axis_index("rows")
    z, core = rows // 2, rows % 2
    x, y = owner % X, owner // X
    barrier = pltpu.get_barrier_semaphore()
    first_core, second_core = core == 0, core == 1
    mx = (mx0, mx1, mx2)

    column = [(rows + d) % NR for d in range(1, NR)]
    chips = [(z + d) % Z for d in range(1, Z)]
    across_x = [y * X + (x + d) % X for d in range(1, X)]
    across_y = [((y + d) % Y) * X + x for d in range(1, Y)]
    right = ((z + 1) % Z) * 2 + core
    left = ((z + Z - 1) % Z) * 2 + core
    partner = z * 2 + 1 - core

    def remote(src, dst, send, recv, **where):
        return pltpu.make_async_remote_copy(
            src_ref=src, dst_ref=dst, send_sem=send, recv_sem=recv,
            device_id=where, device_id_type=MESH)

    def signal(sem, **where):
        pl.semaphore_signal(sem, inc=1, device_id=where, device_id_type=MESH)

    for c in chips:
        signal(barrier, rows=c * 2)

    @pl.when(second_core)
    def _():
        signal(barrier, rows=partner)
        for o in across_x + across_y:
            signal(barrier, owner=o)

    spans = [(e, b * LANES, n * LANES) for e, b, n in PIECES]
    loads = [
        pltpu.make_async_copy(w_hbm.at[e, pl.ds(a, n)], w.at[e, pl.ds(a, n)], in_sem.at[i])
        for i, (e, a, n) in enumerate(spans)
    ]
    loads.append(pltpu.make_async_copy(rw_hbm, rw, in_sem.at[3]))
    loads.append(pltpu.make_async_copy(gain_hbm, gain, in_sem.at[4]))
    for load in loads:
        load.start()

    def maxima(i):
        loads[i].wait()
        e, first, n = PIECES[i]
        for b in range(n):
            block = jnp.abs(w[e, (first + b) * LANES:(first + b + 1) * LANES, :])
            mx[i][rows, b:b + 1, :] = jnp.max(block.T, axis=0, keepdims=True)

    def mx_copies(i):
        return [
            remote(mx[i].at[rows], mx[i].at[rows], mx_send.at[i, s], mx_recv.at[i, rows], rows=r)
            for s, r in enumerate(column)
        ]

    sent = [mx_copies(i) for i in range(3)]
    maxima(0)

    @pl.when(first_core)
    def _():
        pl.semaphore_wait(barrier, NR - 1)
        signal(go, rows=partner)

    @pl.when(second_core)
    def _():
        pl.semaphore_wait(go, 1)

    for copy in sent[0]:
        copy.start()
    for i in (1, 2):
        maxima(i)
        for copy in sent[i]:
            copy.start()

    loads[3].wait()
    loads[4].wait()
    piece = (rw[...] * gain[...]).astype(BF16)
    mine[...] = piece
    r1 = [remote(mine, rb.at[owner, rows], r1_send.at[s], r1_recv.at[rows], rows=c * 2 + 1) for s, c in enumerate(chips)]
    r1_die = remote(mine, rb.at[owner, rows], r1_send.at[Z - 1], r1_recv.at[rows], rows=partner)
    for copy in r1:
        copy.start()

    @pl.when(first_core)
    def _():
        r1_die.start()

    @pl.when(second_core)
    def _():
        rb[owner, rows] = piece

    def cells(origin, k):
        e, first, n, _ = CHUNKS[k]
        lanes = pl.multiple_of(origin * LANES, LANES)
        return out.at[e, pl.ds(first * LANES, n * LANES), pl.ds(lanes, LANES)]

    def ring(side, origin, k, sent_at, recv_at):
        part = cells(origin, k)
        recv = (right_recv, left_recv)[side]
        return remote(part, part, ring_send.at[side, sent_at], recv.at[recv_at], rows=(right, left)[side])

    def die(side, origin, k, j):
        part = cells(origin, k)
        return remote(part, part, die_send.at[side, j], die_recv.at[side, j], rows=partner)

    def die_own(origin, k):
        part = cells(origin, k)
        return remote(part, part, own_send.at[k], own_recv.at[k], rows=partner)

    def scaled(i):
        for s, r in enumerate(column):
            remote(mx[i].at[r], mx[i].at[r], mx_send.at[i, s], mx_recv.at[i, r], rows=r).wait_recv()
        scale = jnp.max(mx[i][...], axis=0)
        e, first, n = PIECES[i]
        for b in range(n):
            scale_out[e:e + 1, (first + b) * LANES:(first + b + 1) * LANES] = scale[b:b + 1]
        return 1.0 / scale

    inv = None
    held = -1
    for k, (e, first, n, i) in enumerate(CHUNKS):
        if i != held:
            inv, held = scaled(i), i
        skip = first - PIECES[i][1]
        lanes = pl.ds(pl.multiple_of(rows * LANES, LANES), LANES)
        for b in range(n):
            factor = jnp.broadcast_to(inv[skip + b:skip + b + 1], (LANES, LANES)).T
            span = slice((first + b) * LANES, (first + b + 1) * LANES)
            out[e, span, lanes] = (w[e, span, :] * factor).astype(BF16)
        for side in range(2):
            ring(side, rows, k, k, k).start()
        die_own(rows, k).start()

    def origin_of(side, d, c):
        step = (Z - 1 - d) if side == 0 else (d + 1)
        return ((z + step) % Z) * 2 + c

    def arrive(j):
        for side in range(2):
            d, k = ARRIVALS[side][j]
            origin = origin_of(side, d, core)
            ring(side, origin, k, j, j).wait_recv()
            onward = [(d + 1, k)] if d < 2 else []
            if d == 2:
                onward = {(0, 1): [(3, 1), (3, 0)], (1, 2): [(3, 2)], (1, 3): [(3, 3)]}.get((side, k), [])
            for to in onward:
                at = ARRIVALS[side].index(to)
                ring(side, origin, to[1], at, at).start()
            die(side, origin, k, j).start()

    rx = [remote(rb.at[owner], rb.at[owner], rx_send.at[s], rx_recv.at[x], owner=o) for s, o in enumerate(across_x)]
    band = rb.at[pl.ds(y * X, X)]
    ry = [remote(band, band, ry_send.at[s], ry_recv.at[y], owner=o) for s, o in enumerate(across_y)]
    rd = remote(rb, rb, rd_send, rd_recv, rows=partner)

    def router_x():
        @pl.when(second_core)
        def _():
            for s, r in enumerate(column):
                remote(mine, rb.at[owner, r], r1_send.at[0], r1_recv.at[r], rows=r).wait_recv()
            pl.semaphore_wait(barrier, len(across_x) + len(across_y))
            for copy in rx:
                copy.start()

    def router_y():
        @pl.when(second_core)
        def _():
            for o in across_x:
                remote(rb.at[o], rb.at[o], rx_send.at[0], rx_recv.at[o % X], owner=o).wait_recv()
            for copy in ry:
                copy.start()

    def router_die():
        @pl.when(second_core)
        def _():
            for o in across_y:
                theirs = rb.at[pl.ds((o // X) * X, X)]
                remote(theirs, theirs, ry_send.at[0], ry_recv.at[o // X], owner=o).wait_recv()
            rd.start()

    def router_end():
        @pl.when(first_core)
        def _():
            rd.wait_recv()

        for o in range(X * Y):
            for r in range(NR):
                router_out[2 * o:2 * o + 2, r * LANES:(r + 1) * LANES] = rb[o, r]

    between = {4: router_x, 6: router_y, 8: router_die, 10: router_end}
    for j in range(STEPS):
        if j in between:
            between[j]()
        arrive(j)

    for k in range(K):
        die_own(partner, k).wait_recv()
        die_own(rows, k).wait_send()
    for j in range(STEPS):
        for side in range(2):
            d, k = ARRIVALS[side][j]
            die(side, origin_of(side, d, 1 - core), k, j).wait_recv()
    for j in range(STEPS):
        for side in range(2):
            d, k = ARRIVALS[side][j]
            die(side, origin_of(side, d, core), k, j).wait_send()
    for side in range(2):
        for k in range(K):
            ring(side, rows, k, k, k).wait_send()
        for at in range(K, STEPS):
            d, k = ARRIVALS[side][at]
            ring(side, origin_of(side, d - 1, core), k, at, at).wait_send()
    for copies in sent:
        for copy in copies:
            copy.wait_send()
    for copy in r1:
        copy.wait_send()

    @pl.when(first_core)
    def _():
        r1_die.wait_send()

    @pl.when(second_core)
    def _():
        for copy in rx + ry + [rd]:
            copy.wait_send()


PARTS = 11


def write(a, b, c, a_out, b_out, c_out, sems):
    tall = ROWS // PARTS
    copies = [
        pltpu.make_async_copy(a.at[e, pl.ds(i * tall, tall)], a_out.at[e, pl.ds(i * tall, tall)], sems.at[e * PARTS + i])
        for e in range(E) for i in range(PARTS)
    ]
    copies.append(pltpu.make_async_copy(b, b_out, sems.at[E * PARTS]))
    copies.append(pltpu.make_async_copy(c, c_out, sems.at[E * PARTS + 1]))
    for copy in copies:
        copy.start()
    for copy in copies:
        copy.wait()


def on_device(w_down, router_weight, router_gain):
    dma = pltpu.SemaphoreType.DMA
    shapes = (
        jax.ShapeDtypeStruct((E, ROWS, NR * LANES), BF16),
        jax.ShapeDtypeStruct((E, ROWS), F32),
        jax.ShapeDtypeStruct((E * X * Y, NR * LANES), BF16),
    )
    args = (w_down, router_weight.T, router_gain[None, :])
    held = pl.pallas_call(
        kernel,
        name="serve",
        out_shape=shapes,
        in_specs=[pl.BlockSpec(memory_space=pltpu.HBM)] * 3,
        out_specs=(pl.BlockSpec(memory_space=pltpu.VMEM),) * 3,
        scratch_shapes=[
            pltpu.VMEM((E, ROWS, LANES), F32),
            pltpu.VMEM((2, LANES), F32),
            pltpu.VMEM((1, LANES), F32),
            *[pltpu.VMEM((NR, n, LANES), F32) for _, _, n in PIECES],
            pltpu.VMEM((2, LANES), BF16),
            pltpu.VMEM((X * Y, NR, 2, LANES), BF16),
            dma((5,)), pltpu.SemaphoreType.REGULAR, dma((3, NR - 1)), dma((3, NR)),
            dma((2, STEPS)), dma((STEPS,)), dma((STEPS,)),
            dma((2, STEPS)), dma((2, STEPS)), dma((K,)), dma((K,)),
            dma((Z,)), dma((NR,)), dma((X - 1,)), dma((X,)), dma((Y - 1,)), dma((Y,)), dma(()), dma(()),
        ],
        compiler_params=pltpu.CompilerParams(
            collective_id=0, has_side_effects=True, vmem_limit_bytes=24 * 1024 * 1024
        ),
    )(*(pltpu.with_memory_space_constraint(a, pltpu.HBM) for a in args))
    out, scale, router = pl.pallas_call(
        write,
        name="write",
        out_shape=shapes,
        in_specs=[pl.BlockSpec(memory_space=pltpu.VMEM)] * 3,
        out_specs=(pl.BlockSpec(memory_space=pltpu.HBM),) * 3,
        scratch_shapes=[dma((E * PARTS + 2,))],
        compiler_params=pltpu.CompilerParams(vmem_limit_bytes=24 * 1024 * 1024),
    )(*held)
    return out, scale, router.T


def solution(mesh):
    placed = (P("owner", None, "rows"), P("rows", "owner"), P("rows"))
    return jax.shard_map(
        on_device,
        mesh=mesh,
        in_specs=placed,
        out_specs=(P("owner", None, None), P("owner", None), P()),
        check_vma=False,
    )
```

```python
import jax
import jax.numpy as jnp
from jax import lax
from jax.experimental import pallas as pl
from jax.experimental.pallas import tpu as pltpu
from jax.sharding import PartitionSpec as P

MESH = pl.DeviceIdType.MESH
BF16 = jnp.bfloat16
F32 = jnp.float32

E = 2
ROWS = 1408
LANES = 128
Z = 8
NR = 16
X, Y = 4, 8
BLOCKS = ROWS // LANES
HALF = 6
CHUNKS = ((0, 0, 3), (0, 3, 8), (1, 0, 8), (1, 8, 3))
K = len(CHUNKS)
RAW = CHUNKS[0][2] * LANES
NEAR = ((0, 1), (1, 0), (0, 2), (0, 3), (1, 1), (2, 0), (1, 2), (1, 3), (2, 1), (2, 2), (2, 3))
ARRIVALS = (NEAR + ((3, 1), (3, 0)), NEAR + ((3, 2), (3, 3)))
FAR = ({1: ((3, 1), (3, 0))}, {2: ((3, 2),), 3: ((3, 3),)})


def kernel(w_hbm, rw_hbm, gain_hbm, out, scale_out, router_out,
           w, rw, gain, mx, half, swapped, reduced, final, raw, mine, rb,
           in_sem, go, mx_send, mx_recv, sw_send, sw_recv, red_send, red_recv, fin_send, fin_recv,
           raw_send, raw_recv, ring_send, right_recv, left_recv,
           die_send, die_recv, own_send, own_recv,
           r1_send, r1_recv, rx_send, rx_recv, ry_send, ry_recv, rd_send, rd_recv):
    owner = lax.axis_index("owner")
    rows = lax.axis_index("rows")
    z, core = rows // 2, rows % 2
    x, y = owner % X, owner // X
    barrier = pltpu.get_barrier_semaphore()
    first_core, second_core = core == 0, core == 1

    column = [(rows + d) % NR for d in range(1, NR)]
    chips = [(z + d) % Z for d in range(1, Z)]
    across_x = [y * X + (x + d) % X for d in range(1, X)]
    across_y = [((y + d) % Y) * X + x for d in range(1, Y)]
    sides = (((z + 1) % Z) * 2 + core, ((z + Z - 1) % Z) * 2 + core)
    partner = z * 2 + 1 - core

    def remote(src, dst, send, recv, **where):
        return pltpu.make_async_remote_copy(
            src_ref=src, dst_ref=dst, send_sem=send, recv_sem=recv,
            device_id=where, device_id_type=MESH)

    def signal(sem, **where):
        pl.semaphore_signal(sem, inc=1, device_id=where, device_id_type=MESH)

    for c in chips:
        signal(barrier, rows=c * 2)

    @pl.when(second_core)
    def _():
        signal(barrier, rows=partner)
        for o in across_x + across_y:
            signal(barrier, owner=o)

    loads = [pltpu.make_async_copy(w_hbm.at[e], w.at[e], in_sem.at[e]) for e in range(E)]
    loads.append(pltpu.make_async_copy(rw_hbm, rw, in_sem.at[2]))
    loads.append(pltpu.make_async_copy(gain_hbm, gain, in_sem.at[3]))
    for load in loads:
        load.start()

    def span(b):
        return slice(b * LANES, (b + 1) * LANES)

    def maximum(e, b):
        return jnp.max(jnp.abs(w[e, span(b), :]).T, axis=0, keepdims=True)

    loads[0].wait()
    for b in range(BLOCKS):
        mx[rows, b:b + 1, :] = maximum(0, b)

    @pl.when(first_core)
    def _():
        pl.semaphore_wait(barrier, NR - 1)
        signal(go, rows=partner)

    @pl.when(second_core)
    def _():
        pl.semaphore_wait(go, 1)

    mx_sent = [remote(mx.at[rows], mx.at[rows], mx_send.at[s], mx_recv.at[rows], rows=r) for s, r in enumerate(column)]
    for copy in mx_sent:
        copy.start()
    raw_sent = [
        remote(w.at[0, pl.ds(0, RAW)], raw.at[side], raw_send.at[side], raw_recv.at[side], rows=sides[side])
        for side in range(2)
    ]
    for copy in raw_sent:
        copy.start()

    loads[1].wait()
    for b in range(BLOCKS):
        top = maximum(1, b)
        for h, first in enumerate((0, BLOCKS - HALF)):
            if first <= b < first + HALF:
                half[h, b - first:b - first + 1, :] = top
    swap = remote(half.at[1 - core], swapped, sw_send, sw_recv, rows=partner)
    swap.start()

    loads[2].wait()
    loads[3].wait()
    piece = (rw[...] * gain[...]).astype(BF16)
    mine[...] = piece
    r1 = [remote(mine, rb.at[owner, rows], r1_send.at[s], r1_recv.at[rows], rows=c * 2 + 1) for s, c in enumerate(chips)]
    r1_die = remote(mine, rb.at[owner, rows], r1_send.at[Z - 1], r1_recv.at[rows], rows=partner)
    for copy in r1:
        copy.start()

    @pl.when(first_core)
    def _():
        r1_die.start()

    @pl.when(second_core)
    def _():
        rb[owner, rows] = piece

    swap.wait_recv()
    reduced[z] = jnp.maximum(half[core], swapped[...])
    red_sent = [remote(reduced.at[z], reduced.at[z], red_send.at[s], red_recv.at[z], rows=c * 2 + core) for s, c in enumerate(chips)]
    for copy in red_sent:
        copy.start()

    def cells(origin, k):
        e, first, n = CHUNKS[k]
        lanes = pl.multiple_of(origin * LANES, LANES)
        return out.at[e, pl.ds(first * LANES, n * LANES), pl.ds(lanes, LANES)]

    def ring(side, origin, to):
        d, k = to
        part = cells(origin, k)
        recv = (right_recv, left_recv)[side]
        return remote(part, part, ring_send.at[side, d * K + k], recv.at[d * K + k], rows=sides[side])

    def die(side, origin, at):
        d, k = at
        part = cells(origin, k)
        return remote(part, part, die_send.at[side, d * K + k], die_recv.at[side, d * K + k], rows=partner)

    def die_own(origin, k):
        part = cells(origin, k)
        return remote(part, part, own_send.at[k], own_recv.at[k], rows=partner)

    def origin_of(side, d, c):
        step = (Z - 1 - d) if side == 0 else (d + 1)
        return ((z + step) % Z) * 2 + c

    def narrow(values, origin, k, factors):
        e, first, n = CHUNKS[k]
        lanes = pl.ds(pl.multiple_of(origin * LANES, LANES), LANES)
        for b in range(n):
            factor = jnp.broadcast_to(factors[first + b], (LANES, LANES)).T
            out[e, span(first + b), lanes] = (values(e, first + b) * factor).astype(BF16)

    def own(k, factors):
        narrow(lambda e, b: w[e, span(b), :], rows, k, factors)
        if k > 0:
            for side in range(2):
                ring(side, rows, (0, k)).start()
        die_own(rows, k).start()

    def scaled(e, tops):
        for b in range(BLOCKS):
            scale_out[e:e + 1, span(b)] = tops[b]
        return [1.0 / top for top in tops]

    for s, r in enumerate(column):
        remote(mx.at[r], mx.at[r], mx_send.at[s], mx_recv.at[r], rows=r).wait_recv()
    top = jnp.max(mx[...], axis=0)
    factors = scaled(0, [top[b:b + 1] for b in range(BLOCKS)])
    own(1, factors)
    own(0, factors)
    for side in range(2):
        origin = origin_of(side, 0, core)
        raw_sent[side].wait_recv()
        narrow(lambda e, b: raw[side, span(b), :], origin, 0, factors)
        ring(side, origin, (1, 0)).start()
        die(side, origin, (0, 0)).start()

    for s, c in enumerate(chips):
        remote(reduced.at[c], reduced.at[c], red_send.at[s], red_recv.at[c], rows=c * 2 + core).wait_recv()
    final[core] = jnp.max(reduced[...], axis=0)
    share = remote(final.at[core], final.at[core], fin_send, fin_recv, rows=partner)
    share.start()
    remote(final.at[1 - core], final.at[1 - core], fin_send, fin_recv, rows=partner).wait_recv()
    low, high = final[0], final[1]
    tops = [low[b:b + 1] for b in range(HALF)]
    tops += [high[b - BLOCKS + HALF:b - BLOCKS + HALF + 1] for b in range(HALF, BLOCKS)]
    factors = scaled(1, tops)
    own(2, factors)
    own(3, factors)

    def arrive(j):
        for side in range(2):
            d, k = ARRIVALS[side][j]
            origin = origin_of(side, d, core)
            ring(side, origin, (d, k)).wait_recv()
            onward = ((d + 1, k),) if d < 2 else FAR[side].get(k, ()) if d == 2 else ()
            for to in onward:
                ring(side, origin, to).start()
            die(side, origin, (d, k)).start()

    rx = [remote(rb.at[owner], rb.at[owner], rx_send.at[s], rx_recv.at[x], owner=o) for s, o in enumerate(across_x)]
    band = rb.at[pl.ds(y * X, X)]
    ry = [remote(band, band, ry_send.at[s], ry_recv.at[y], owner=o) for s, o in enumerate(across_y)]
    rd = remote(rb, rb, rd_send, rd_recv, rows=partner)

    def router_x():
        @pl.when(second_core)
        def _():
            for s, r in enumerate(column):
                remote(mine, rb.at[owner, r], r1_send.at[0], r1_recv.at[r], rows=r).wait_recv()
            pl.semaphore_wait(barrier, len(across_x) + len(across_y))
            for copy in rx:
                copy.start()

    def router_y():
        @pl.when(second_core)
        def _():
            for o in across_x:
                remote(rb.at[o], rb.at[o], rx_send.at[0], rx_recv.at[o % X], owner=o).wait_recv()
            for copy in ry:
                copy.start()

    def router_die():
        @pl.when(second_core)
        def _():
            for o in across_y:
                theirs = rb.at[pl.ds((o // X) * X, X)]
                remote(theirs, theirs, ry_send.at[0], ry_recv.at[o // X], owner=o).wait_recv()
            rd.start()

    def router_end():
        @pl.when(first_core)
        def _():
            rd.wait_recv()

        for o in range(X * Y):
            for r in range(NR):
                router_out[2 * o:2 * o + 2, r * LANES:(r + 1) * LANES] = rb[o, r]

    between = {3: router_x, 5: router_y, 7: router_die, 9: router_end}
    for j in range(len(NEAR) + 2):
        if j in between:
            between[j]()
        arrive(j)

    for k in range(K):
        die_own(partner, k).wait_recv()
    for side in range(2):
        for d, k in ((0, 0),) + ARRIVALS[side]:
            die(side, origin_of(side, d, 1 - core), (d, k)).wait_recv()
    for k in range(K):
        die_own(rows, k).wait_send()
    for side in range(2):
        raw_sent[side].wait_send()
        die(side, origin_of(side, 0, core), (0, 0)).wait_send()
        for d, k in ARRIVALS[side]:
            die(side, origin_of(side, d, core), (d, k)).wait_send()
            ring(side, origin_of(side, d - 1, core), (d, k)).wait_send()
    for copy in mx_sent + red_sent + r1 + [swap, share]:
        copy.wait_send()

    @pl.when(first_core)
    def _():
        r1_die.wait_send()

    @pl.when(second_core)
    def _():
        for copy in rx + ry + [rd]:
            copy.wait_send()


PARTS = 11


def write(a, b, c, a_out, b_out, c_out, sems):
    tall = ROWS // PARTS
    copies = [
        pltpu.make_async_copy(a.at[e, pl.ds(i * tall, tall)], a_out.at[e, pl.ds(i * tall, tall)], sems.at[e * PARTS + i])
        for e in range(E) for i in range(PARTS)
    ]
    copies.append(pltpu.make_async_copy(b, b_out, sems.at[E * PARTS]))
    copies.append(pltpu.make_async_copy(c, c_out, sems.at[E * PARTS + 1]))
    for copy in copies:
        copy.start()
    for copy in copies:
        copy.wait()


def on_device(w_down, router_weight, router_gain):
    dma = pltpu.SemaphoreType.DMA
    shapes = (
        jax.ShapeDtypeStruct((E, ROWS, NR * LANES), BF16),
        jax.ShapeDtypeStruct((E, ROWS), F32),
        jax.ShapeDtypeStruct((E * X * Y, NR * LANES), BF16),
    )
    args = (w_down, router_weight.T, router_gain[None, :])
    held = pl.pallas_call(
        kernel,
        name="serve",
        out_shape=shapes,
        in_specs=[pl.BlockSpec(memory_space=pltpu.HBM)] * 3,
        out_specs=(pl.BlockSpec(memory_space=pltpu.VMEM),) * 3,
        scratch_shapes=[
            pltpu.VMEM((E, ROWS, LANES), F32),
            pltpu.VMEM((2, LANES), F32),
            pltpu.VMEM((1, LANES), F32),
            pltpu.VMEM((NR, BLOCKS, LANES), F32),
            pltpu.VMEM((2, HALF, LANES), F32),
            pltpu.VMEM((HALF, LANES), F32),
            pltpu.VMEM((Z, HALF, LANES), F32),
            pltpu.VMEM((2, HALF, LANES), F32),
            pltpu.VMEM((2, RAW, LANES), F32),
            pltpu.VMEM((2, LANES), BF16),
            pltpu.VMEM((X * Y, NR, 2, LANES), BF16),
            dma((4,)), pltpu.SemaphoreType.REGULAR, dma((NR - 1,)), dma((NR,)),
            dma(()), dma(()), dma((Z - 1,)), dma((Z,)), dma(()), dma(()),
            dma((2,)), dma((2,)), dma((2, 4 * K)), dma((4 * K,)), dma((4 * K,)),
            dma((2, 4 * K)), dma((2, 4 * K)), dma((K,)), dma((K,)),
            dma((Z,)), dma((NR,)), dma((X - 1,)), dma((X,)), dma((Y - 1,)), dma((Y,)), dma(()), dma(()),
        ],
        compiler_params=pltpu.CompilerParams(
            collective_id=0, has_side_effects=True, vmem_limit_bytes=24 * 1024 * 1024
        ),
    )(*(pltpu.with_memory_space_constraint(a, pltpu.HBM) for a in args))
    out, scale, router = pl.pallas_call(
        write,
        name="write",
        out_shape=shapes,
        in_specs=[pl.BlockSpec(memory_space=pltpu.VMEM)] * 3,
        out_specs=(pl.BlockSpec(memory_space=pltpu.HBM),) * 3,
        scratch_shapes=[dma((E * PARTS + 2,))],
        compiler_params=pltpu.CompilerParams(vmem_limit_bytes=24 * 1024 * 1024),
    )(*held)
    return out, scale, router.T


def solution(mesh):
    placed = (P("owner", None, "rows"), P("rows", "owner"), P("rows"))
    return jax.shard_map(
        on_device,
        mesh=mesh,
        in_specs=placed,
        out_specs=(P("owner", None, None), P("owner", None), P()),
        check_vma=False,
    )
```

```python
import jax
import jax.numpy as jnp
from jax import lax
from jax.experimental import pallas as pl
from jax.experimental.pallas import tpu as pltpu
from jax.sharding import PartitionSpec as P

MESH = pl.DeviceIdType.MESH
BF16 = jnp.bfloat16
F32 = jnp.float32

E = 2
ROWS = 1408
LANES = 128
Z = 8
NR = 16
X, Y = 4, 8
BLOCKS = ROWS // LANES
HALF = 6
CHUNKS = ((0, 0, 3), (0, 3, 8), (1, 0, 8), (1, 8, 3))
K = len(CHUNKS)
RAW = CHUNKS[0][2] * LANES
NEAR = ((0, 1), (1, 0), (0, 2), (0, 3), (1, 1), (2, 0), (1, 2), (1, 3), (2, 1), (2, 2), (2, 3))
ARRIVALS = (NEAR + ((3, 1), (3, 0)), NEAR + ((3, 2), (3, 3)))
STEPS = len(NEAR) + 2
SETTLED = STEPS - 5
FAR = ({1: ((3, 1), (3, 0))}, {2: ((3, 2),), 3: ((3, 3),)})


def kernel(w_hbm, rw_hbm, gain_hbm, out, scale_out, router_out,
           w, rw, gain, mx, cross, both, half, swapped, reduced, final, raw, mine, rb,
           in_sem, go, mx_send, mx_recv, both_send, both_recv, sw_send, sw_recv, red_send, red_recv, fin_send, fin_recv,
           raw_send, raw_recv, ring_send, right_recv, left_recv,
           die_send, die_recv, own_send, own_recv,
           r1_send, r1_recv, rx_send, rx_recv, ry_send, ry_recv, rd_send, rd_recv):
    owner = lax.axis_index("owner")
    rows = lax.axis_index("rows")
    z, core = rows // 2, rows % 2
    x, y = owner % X, owner // X
    barrier = pltpu.get_barrier_semaphore()
    first_core, second_core = core == 0, core == 1

    chips = [(z + d) % Z for d in (4, 3, 5, 2, 6, 1, 7)]
    column = [(rows + d) % NR for d in range(1, NR)]
    across_x = [y * X + (x + d) % X for d in range(1, X)]
    across_y = [((y + d) % Y) * X + x for d in range(1, Y)]
    sides = (((z + 1) % Z) * 2 + core, ((z + Z - 1) % Z) * 2 + core)
    partner = z * 2 + 1 - core

    def remote(src, dst, send, recv, **where):
        return pltpu.make_async_remote_copy(
            src_ref=src, dst_ref=dst, send_sem=send, recv_sem=recv,
            device_id=where, device_id_type=MESH)

    def signal(sem, **where):
        pl.semaphore_signal(sem, inc=1, device_id=where, device_id_type=MESH)

    for c in chips:
        signal(barrier, rows=c * 2)

    @pl.when(second_core)
    def _():
        signal(barrier, rows=partner)
        for o in across_x + across_y:
            signal(barrier, owner=o)

    loads = [pltpu.make_async_copy(w_hbm.at[e], w.at[e], in_sem.at[e]) for e in range(E)]
    loads.append(pltpu.make_async_copy(rw_hbm, rw, in_sem.at[2]))
    loads.append(pltpu.make_async_copy(gain_hbm, gain, in_sem.at[3]))
    for load in loads:
        load.start()

    def span(b):
        return slice(b * LANES, (b + 1) * LANES)

    def maximum(e, b):
        return jnp.max(jnp.abs(w[e, span(b), :]).T, axis=0, keepdims=True)

    loads[0].wait()
    for b in range(BLOCKS):
        mx[z, b:b + 1, :] = maximum(0, b)

    @pl.when(first_core)
    def _():
        pl.semaphore_wait(barrier, NR - 1)
        signal(go, rows=partner)

    @pl.when(second_core)
    def _():
        pl.semaphore_wait(go, 1)

    mx_sent = [remote(mx.at[z], mx.at[z], mx_send.at[s], mx_recv.at[z], rows=c * 2 + core) for s, c in enumerate(chips)]
    mx_sent.insert(1, remote(mx.at[z], cross, mx_send.at[Z - 1], mx_recv.at[Z], rows=chips[0] * 2 + 1 - core))
    for copy in mx_sent:
        copy.start()
    raw_sent = [
        remote(w.at[0, pl.ds(0, RAW)], raw.at[side], raw_send.at[side], raw_recv.at[side], rows=sides[side])
        for side in range(2)
    ]
    for copy in raw_sent:
        copy.start()

    loads[1].wait()
    for b in range(BLOCKS):
        top = maximum(1, b)
        for h, first in enumerate((0, BLOCKS - HALF)):
            if first <= b < first + HALF:
                half[h, b - first:b - first + 1, :] = top
    swap = remote(half.at[1 - core], swapped, sw_send, sw_recv, rows=partner)
    swap.start()

    loads[2].wait()
    loads[3].wait()
    piece = (rw[...] * gain[...]).astype(BF16)
    mine[...] = piece
    r1 = [remote(mine, rb.at[owner, rows], r1_send.at[s], r1_recv.at[rows], rows=c * 2 + 1) for s, c in enumerate(chips)]
    r1_die = remote(mine, rb.at[owner, rows], r1_send.at[Z - 1], r1_recv.at[rows], rows=partner)
    for copy in r1:
        copy.start()

    @pl.when(first_core)
    def _():
        r1_die.start()

    @pl.when(second_core)
    def _():
        rb[owner, rows] = piece

    swap.wait_recv()
    reduced[z] = jnp.maximum(half[core], swapped[...])
    red_sent = [remote(reduced.at[z], reduced.at[z], red_send.at[s], red_recv.at[z], rows=c * 2 + core) for s, c in enumerate(chips)]
    for copy in red_sent:
        copy.start()

    def cells(origin, k):
        e, first, n = CHUNKS[k]
        lanes = pl.multiple_of(origin * LANES, LANES)
        return out.at[e, pl.ds(first * LANES, n * LANES), pl.ds(lanes, LANES)]

    def ring(side, origin, to):
        d, k = to
        part = cells(origin, k)
        recv = (right_recv, left_recv)[side]
        return remote(part, part, ring_send.at[side, d * K + k], recv.at[d * K + k], rows=sides[side])

    def die(side, origin, at):
        d, k = at
        part = cells(origin, k)
        return remote(part, part, die_send.at[side, d * K + k], die_recv.at[side, d * K + k], rows=partner)

    def die_own(origin, k):
        part = cells(origin, k)
        return remote(part, part, own_send.at[k], own_recv.at[k], rows=partner)

    def origin_of(side, d, c):
        step = (Z - 1 - d) if side == 0 else (d + 1)
        return ((z + step) % Z) * 2 + c

    def narrow(values, origin, k, factors):
        e, first, n = CHUNKS[k]
        lanes = pl.ds(pl.multiple_of(origin * LANES, LANES), LANES)
        for b in range(n):
            factor = jnp.broadcast_to(factors[first + b], (LANES, LANES)).T
            out[e, span(first + b), lanes] = (values(e, first + b) * factor).astype(BF16)

    def own(k, factors):
        narrow(lambda e, b: w[e, span(b), :], rows, k, factors)
        if k > 0:
            for side in range(2):
                ring(side, rows, (0, k)).start()
        die_own(rows, k).start()

    def scaled(e, tops):
        for b in range(BLOCKS):
            scale_out[e:e + 1, span(b)] = tops[b]
        return [1.0 / top for top in tops]

    def mx_wait(s, c):
        remote(mx.at[c], mx.at[c], mx_send.at[s], mx_recv.at[c], rows=c * 2 + core).wait_recv()

    near = mx[z]
    for s, c in list(enumerate(chips))[:0:-1]:
        mx_wait(s, c)
        near = jnp.maximum(near, mx[c])
    both[core] = near
    meet = remote(both.at[core], both.at[core], both_send, both_recv, rows=partner)
    meet.start()
    mx_wait(0, chips[0])
    remote(cross, cross, mx_send.at[Z - 1], mx_recv.at[Z], rows=partner).wait_recv()
    remote(both.at[1 - core], both.at[1 - core], both_send, both_recv, rows=partner).wait_recv()
    top = jnp.maximum(jnp.maximum(both[0], both[1]), jnp.maximum(mx[chips[0]], cross[...]))
    factors = scaled(0, [top[b:b + 1] for b in range(BLOCKS)])
    own(1, factors)
    own(0, factors)
    for side in range(2):
        origin = origin_of(side, 0, core)
        raw_sent[side].wait_recv()
        narrow(lambda e, b: raw[side, span(b), :], origin, 0, factors)
        ring(side, origin, (1, 0)).start()
        die(side, origin, (0, 0)).start()

    for s, c in enumerate(chips):
        remote(reduced.at[c], reduced.at[c], red_send.at[s], red_recv.at[c], rows=c * 2 + core).wait_recv()
    final[core] = jnp.max(reduced[...], axis=0)
    share = remote(final.at[core], final.at[core], fin_send, fin_recv, rows=partner)
    share.start()
    remote(final.at[1 - core], final.at[1 - core], fin_send, fin_recv, rows=partner).wait_recv()
    low, high = final[0], final[1]
    tops = [low[b:b + 1] for b in range(HALF)]
    tops += [high[b - BLOCKS + HALF:b - BLOCKS + HALF + 1] for b in range(HALF, BLOCKS)]
    factors = scaled(1, tops)
    own(2, factors)
    own(3, factors)

    def arrive(j):
        for side in range(2):
            d, k = ARRIVALS[side][j]
            origin = origin_of(side, d, core)
            ring(side, origin, (d, k)).wait_recv()
            onward = ((d + 1, k),) if d < 2 else FAR[side].get(k, ()) if d == 2 else ()
            for to in onward:
                ring(side, origin, to).start()
            die(side, origin, (d, k)).start()

    rx = [remote(rb.at[owner], rb.at[owner], rx_send.at[s], rx_recv.at[x], owner=o) for s, o in enumerate(across_x)]
    band = rb.at[pl.ds(y * X, X)]
    ry = [remote(band, band, ry_send.at[s], ry_recv.at[y], owner=o) for s, o in enumerate(across_y)]
    rd = remote(rb, rb, rd_send, rd_recv, rows=partner)

    def router_x():
        @pl.when(second_core)
        def _():
            for s, r in enumerate(column):
                remote(mine, rb.at[owner, r], r1_send.at[0], r1_recv.at[r], rows=r).wait_recv()
            pl.semaphore_wait(barrier, len(across_x) + len(across_y))
            for copy in rx:
                copy.start()

    def router_y():
        @pl.when(second_core)
        def _():
            for o in across_x:
                remote(rb.at[o], rb.at[o], rx_send.at[0], rx_recv.at[o % X], owner=o).wait_recv()
            for copy in ry:
                copy.start()

    def router_die():
        @pl.when(second_core)
        def _():
            for o in across_y:
                theirs = rb.at[pl.ds((o // X) * X, X)]
                remote(theirs, theirs, ry_send.at[0], ry_recv.at[o // X], owner=o).wait_recv()
            rd.start()

    def router_end():
        @pl.when(first_core)
        def _():
            rd.wait_recv()

        for o in range(X * Y):
            for r in range(NR):
                router_out[2 * o:2 * o + 2, r * LANES:(r + 1) * LANES] = rb[o, r]

    between = {3: router_x, 5: router_y, 7: router_die, 9: router_end}
    def settle(side, at):
        d, k = at
        die(side, origin_of(side, d, 1 - core), at).wait_recv()
        die(side, origin_of(side, d, core), at).wait_send()

    def sent(side, at):
        d, k = at
        ring(side, origin_of(side, d - 1, core), at).wait_send()

    def settle_early():
        for k in range(K):
            die_own(partner, k).wait_recv()
            die_own(rows, k).wait_send()
        for side in range(2):
            raw_sent[side].wait_send()
            for at in ((0, 0),) + ARRIVALS[side][:SETTLED]:
                settle(side, at)
            for at in ARRIVALS[side]:
                if at[0] < 2:
                    sent(side, at)
        for copy in mx_sent + red_sent + r1 + [swap, share, meet]:
            copy.wait_send()

        @pl.when(first_core)
        def _():
            r1_die.wait_send()

        @pl.when(second_core)
        def _():
            for copy in rx + ry + [rd]:
                copy.wait_send()

    for j in range(STEPS):
        if j in between:
            between[j]()
        if j == STEPS - 2:
            settle_early()
        arrive(j)

    for side in range(2):
        for at in ARRIVALS[side][SETTLED:]:
            settle(side, at)
        for at in ARRIVALS[side]:
            if at[0] >= 2:
                sent(side, at)


PARTS = 2


def write(a, b, c, a_out, b_out, c_out, sems):
    tall = ROWS // PARTS
    copies = [
        pltpu.make_async_copy(a.at[e, pl.ds(i * tall, tall)], a_out.at[e, pl.ds(i * tall, tall)], sems.at[e * PARTS + i])
        for e in range(E) for i in range(PARTS)
    ]
    copies.append(pltpu.make_async_copy(b, b_out, sems.at[E * PARTS]))
    copies.append(pltpu.make_async_copy(c, c_out, sems.at[E * PARTS + 1]))
    for copy in copies:
        copy.start()
    for copy in copies:
        copy.wait()


def on_device(w_down, router_weight, router_gain):
    dma = pltpu.SemaphoreType.DMA
    shapes = (
        jax.ShapeDtypeStruct((E, ROWS, NR * LANES), BF16),
        jax.ShapeDtypeStruct((E, ROWS), F32),
        jax.ShapeDtypeStruct((E * X * Y, NR * LANES), BF16),
    )
    args = (w_down, router_weight.T, router_gain[None, :])
    held = pl.pallas_call(
        kernel,
        name="serve",
        out_shape=shapes,
        in_specs=[pl.BlockSpec(memory_space=pltpu.HBM)] * 3,
        out_specs=(pl.BlockSpec(memory_space=pltpu.VMEM),) * 3,
        scratch_shapes=[
            pltpu.VMEM((E, ROWS, LANES), F32),
            pltpu.VMEM((2, LANES), F32),
            pltpu.VMEM((1, LANES), F32),
            pltpu.VMEM((Z, BLOCKS, LANES), F32),
            pltpu.VMEM((BLOCKS, LANES), F32),
            pltpu.VMEM((2, BLOCKS, LANES), F32),
            pltpu.VMEM((2, HALF, LANES), F32),
            pltpu.VMEM((HALF, LANES), F32),
            pltpu.VMEM((Z, HALF, LANES), F32),
            pltpu.VMEM((2, HALF, LANES), F32),
            pltpu.VMEM((2, RAW, LANES), F32),
            pltpu.VMEM((2, LANES), BF16),
            pltpu.VMEM((X * Y, NR, 2, LANES), BF16),
            dma((4,)), pltpu.SemaphoreType.REGULAR, dma((Z,)), dma((Z + 1,)), dma(()), dma(()),
            dma(()), dma(()), dma((Z - 1,)), dma((Z,)), dma(()), dma(()),
            dma((2,)), dma((2,)), dma((2, 4 * K)), dma((4 * K,)), dma((4 * K,)),
            dma((2, 4 * K)), dma((2, 4 * K)), dma((K,)), dma((K,)),
            dma((Z,)), dma((NR,)), dma((X - 1,)), dma((X,)), dma((Y - 1,)), dma((Y,)), dma(()), dma(()),
        ],
        compiler_params=pltpu.CompilerParams(
            collective_id=0, has_side_effects=True, vmem_limit_bytes=24 * 1024 * 1024
        ),
    )(*(pltpu.with_memory_space_constraint(a, pltpu.HBM) for a in args))
    out, scale, router = pl.pallas_call(
        write,
        name="write",
        out_shape=shapes,
        in_specs=[pl.BlockSpec(memory_space=pltpu.VMEM)] * 3,
        out_specs=(pl.BlockSpec(memory_space=pltpu.HBM),) * 3,
        scratch_shapes=[dma((E * PARTS + 2,))],
        compiler_params=pltpu.CompilerParams(vmem_limit_bytes=24 * 1024 * 1024),
    )(*held)
    return out, scale, router.T


def solution(mesh):
    placed = (P("owner", None, "rows"), P("rows", "owner"), P("rows"))
    return jax.shard_map(
        on_device,
        mesh=mesh,
        in_specs=placed,
        out_specs=(P("owner", None, None), P("owner", None), P()),
        check_vma=False,
    )
```

```python
import jax
import jax.numpy as jnp
from jax import lax
from jax.experimental import pallas as pl
from jax.experimental.pallas import tpu as pltpu
from jax.sharding import PartitionSpec as P

MESH = pl.DeviceIdType.MESH
BF16 = jnp.bfloat16
F32 = jnp.float32

E = 2
ROWS = 1408
LANES = 128
Z = 8
NR = 16
X, Y = 4, 8
BLOCKS = ROWS // LANES
HALF = 6
CHUNKS = ((0, 0, 3), (0, 3, 8), (1, 0, 6), (1, 6, 5))
K = len(CHUNKS)
RAW = CHUNKS[0][2] * LANES
NEAR = ((0, 1), (1, 0), (0, 2), (0, 3), (1, 1), (2, 0), (1, 2), (1, 3), (2, 1), (2, 2), (2, 3))
ARRIVALS = (NEAR + ((3, 1), (3, 0)), NEAR + ((3, 2), (3, 3)))
STEPS = len(NEAR) + 2
SETTLED = STEPS - 5
FAR = ({1: ((3, 1), (3, 0))}, {2: ((3, 2),), 3: ((3, 3),)})


def kernel(w_hbm, rw_hbm, gain_hbm, out, scale_out, router_out,
           w, rw, gain, mx, cross, both, half, swapped, reduced, final, raw, mine, rb,
           in_sem, go, mx_send, mx_recv, both_send, both_recv, sw_send, sw_recv, red_send, red_recv, fin_send, fin_recv,
           raw_send, raw_recv, ring_send, right_recv, left_recv,
           die_send, die_recv, own_send, own_recv,
           r1_send, r1_recv, rx_send, rx_recv, ry_send, ry_recv, rd_send, rd_recv):
    owner = lax.axis_index("owner")
    rows = lax.axis_index("rows")
    z, core = rows // 2, rows % 2
    x, y = owner % X, owner // X
    barrier = pltpu.get_barrier_semaphore()
    first_core, second_core = core == 0, core == 1

    chips = [(z + d) % Z for d in (4, 3, 5, 2, 6, 1, 7)]
    column = [(rows + d) % NR for d in range(1, NR)]
    across_x = [y * X + (x + d) % X for d in range(1, X)]
    across_y = [((y + d) % Y) * X + x for d in range(1, Y)]
    sides = (((z + 1) % Z) * 2 + core, ((z + Z - 1) % Z) * 2 + core)
    partner = z * 2 + 1 - core

    def remote(src, dst, send, recv, **where):
        return pltpu.make_async_remote_copy(
            src_ref=src, dst_ref=dst, send_sem=send, recv_sem=recv,
            device_id=where, device_id_type=MESH)

    def signal(sem, **where):
        pl.semaphore_signal(sem, inc=1, device_id=where, device_id_type=MESH)

    for c in chips:
        signal(barrier, rows=c * 2)

    @pl.when(second_core)
    def _():
        signal(barrier, rows=partner)
        for o in across_x + across_y:
            signal(barrier, owner=o)

    loads = [pltpu.make_async_copy(w_hbm.at[e], w.at[e], in_sem.at[e]) for e in range(E)]
    loads.append(pltpu.make_async_copy(rw_hbm, rw, in_sem.at[2]))
    loads.append(pltpu.make_async_copy(gain_hbm, gain, in_sem.at[3]))
    for load in loads:
        load.start()

    def span(b):
        return slice(b * LANES, (b + 1) * LANES)

    def maximum(e, b):
        return jnp.max(jnp.abs(w[e, span(b), :]).T, axis=0, keepdims=True)

    loads[0].wait()
    for b in range(BLOCKS):
        mx[z, b:b + 1, :] = maximum(0, b)

    @pl.when(first_core)
    def _():
        pl.semaphore_wait(barrier, NR - 1)
        signal(go, rows=partner)

    @pl.when(second_core)
    def _():
        pl.semaphore_wait(go, 1)

    mx_sent = [remote(mx.at[z], mx.at[z], mx_send.at[s], mx_recv.at[z], rows=c * 2 + core) for s, c in enumerate(chips)]
    mx_sent.insert(1, remote(mx.at[z], cross, mx_send.at[Z - 1], mx_recv.at[Z], rows=chips[0] * 2 + 1 - core))
    for copy in mx_sent:
        copy.start()
    raw_sent = [
        remote(w.at[0, pl.ds(0, RAW)], raw.at[side], raw_send.at[side], raw_recv.at[side], rows=sides[side])
        for side in range(2)
    ]
    for copy in raw_sent:
        copy.start()

    loads[1].wait()
    for b in range(BLOCKS):
        top = maximum(1, b)
        for h, first in enumerate((0, BLOCKS - HALF)):
            if first <= b < first + HALF:
                half[h, b - first:b - first + 1, :] = top
    swap = remote(half.at[1 - core], swapped, sw_send, sw_recv, rows=partner)
    swap.start()

    loads[2].wait()
    loads[3].wait()
    piece = (rw[...] * gain[...]).astype(BF16)
    mine[...] = piece
    r1 = [remote(mine, rb.at[owner, rows], r1_send.at[s], r1_recv.at[rows], rows=c * 2 + 1) for s, c in enumerate(chips)]
    r1_die = remote(mine, rb.at[owner, rows], r1_send.at[Z - 1], r1_recv.at[rows], rows=partner)
    for copy in r1:
        copy.start()

    @pl.when(first_core)
    def _():
        r1_die.start()

    @pl.when(second_core)
    def _():
        rb[owner, rows] = piece

    swap.wait_recv()
    reduced[z] = jnp.maximum(half[core], swapped[...])
    red_sent = [remote(reduced.at[z], reduced.at[z], red_send.at[s], red_recv.at[z], rows=c * 2 + core) for s, c in enumerate(chips)]
    for copy in red_sent:
        copy.start()

    def cells(origin, k):
        e, first, n = CHUNKS[k]
        lanes = pl.multiple_of(origin * LANES, LANES)
        return out.at[e, pl.ds(first * LANES, n * LANES), pl.ds(lanes, LANES)]

    def ring(side, origin, to):
        d, k = to
        part = cells(origin, k)
        recv = (right_recv, left_recv)[side]
        return remote(part, part, ring_send.at[side, d * K + k], recv.at[d * K + k], rows=sides[side])

    def die(side, origin, at):
        d, k = at
        part = cells(origin, k)
        return remote(part, part, die_send.at[side, d * K + k], die_recv.at[side, d * K + k], rows=partner)

    def die_own(origin, k):
        part = cells(origin, k)
        return remote(part, part, own_send.at[k], own_recv.at[k], rows=partner)

    def origin_of(side, d, c):
        step = (Z - 1 - d) if side == 0 else (d + 1)
        return ((z + step) % Z) * 2 + c

    def narrow(values, origin, k, factors):
        e, first, n = CHUNKS[k]
        lanes = pl.ds(pl.multiple_of(origin * LANES, LANES), LANES)
        for b in range(n):
            factor = jnp.broadcast_to(factors[first + b], (LANES, LANES)).T
            out[e, span(first + b), lanes] = (values(e, first + b) * factor).astype(BF16)

    def own(k, factors):
        narrow(lambda e, b: w[e, span(b), :], rows, k, factors)
        if k > 0:
            for side in range(2):
                ring(side, rows, (0, k)).start()
        die_own(rows, k).start()

    def scaled(e, tops):
        for b in range(BLOCKS):
            scale_out[e:e + 1, span(b)] = tops[b]
        return [1.0 / top for top in tops]

    def mx_wait(s, c):
        remote(mx.at[c], mx.at[c], mx_send.at[s], mx_recv.at[c], rows=c * 2 + core).wait_recv()

    near = mx[z]
    for s, c in list(enumerate(chips))[:0:-1]:
        mx_wait(s, c)
        near = jnp.maximum(near, mx[c])
    both[core] = near
    meet = remote(both.at[core], both.at[core], both_send, both_recv, rows=partner)
    meet.start()
    mx_wait(0, chips[0])
    remote(cross, cross, mx_send.at[Z - 1], mx_recv.at[Z], rows=partner).wait_recv()
    remote(both.at[1 - core], both.at[1 - core], both_send, both_recv, rows=partner).wait_recv()
    top = jnp.maximum(jnp.maximum(both[0], both[1]), jnp.maximum(mx[chips[0]], cross[...]))
    factors = scaled(0, [top[b:b + 1] for b in range(BLOCKS)])
    own(1, factors)
    own(0, factors)
    for side in range(2):
        origin = origin_of(side, 0, core)
        raw_sent[side].wait_recv()
        narrow(lambda e, b: raw[side, span(b), :], origin, 0, factors)
        ring(side, origin, (1, 0)).start()
        die(side, origin, (0, 0)).start()

    for s, c in enumerate(chips):
        remote(reduced.at[c], reduced.at[c], red_send.at[s], red_recv.at[c], rows=c * 2 + core).wait_recv()
    final[core] = jnp.max(reduced[...], axis=0)
    share = remote(final.at[core], final.at[core], fin_send, fin_recv, rows=partner)
    share.start()
    remote(final.at[1 - core], final.at[1 - core], fin_send, fin_recv, rows=partner).wait_recv()
    low, high = final[0], final[1]
    tops = [low[b:b + 1] for b in range(HALF)]
    tops += [high[b - BLOCKS + HALF:b - BLOCKS + HALF + 1] for b in range(HALF, BLOCKS)]
    factors = scaled(1, tops)
    own(2, factors)
    own(3, factors)

    def arrive(j):
        for side in range(2):
            d, k = ARRIVALS[side][j]
            origin = origin_of(side, d, core)
            ring(side, origin, (d, k)).wait_recv()
            onward = ((d + 1, k),) if d < 2 else FAR[side].get(k, ()) if d == 2 else ()
            for to in onward:
                ring(side, origin, to).start()
            die(side, origin, (d, k)).start()

    rx = [remote(rb.at[owner], rb.at[owner], rx_send.at[s], rx_recv.at[x], owner=o) for s, o in enumerate(across_x)]
    band = rb.at[pl.ds(y * X, X)]
    ry = [remote(band, band, ry_send.at[s], ry_recv.at[y], owner=o) for s, o in enumerate(across_y)]
    rd = remote(rb, rb, rd_send, rd_recv, rows=partner)

    def router_x():
        @pl.when(second_core)
        def _():
            for s, r in enumerate(column):
                remote(mine, rb.at[owner, r], r1_send.at[0], r1_recv.at[r], rows=r).wait_recv()
            pl.semaphore_wait(barrier, len(across_x) + len(across_y))
            for copy in rx:
                copy.start()

    def router_y():
        @pl.when(second_core)
        def _():
            for o in across_x:
                remote(rb.at[o], rb.at[o], rx_send.at[0], rx_recv.at[o % X], owner=o).wait_recv()
            for copy in ry:
                copy.start()

    def router_die():
        @pl.when(second_core)
        def _():
            for o in across_y:
                theirs = rb.at[pl.ds((o // X) * X, X)]
                remote(theirs, theirs, ry_send.at[0], ry_recv.at[o // X], owner=o).wait_recv()
            rd.start()

    def router_end():
        @pl.when(first_core)
        def _():
            rd.wait_recv()

        for o in range(X * Y):
            for r in range(NR):
                router_out[2 * o:2 * o + 2, r * LANES:(r + 1) * LANES] = rb[o, r]

    between = {3: router_x, 5: router_y, 7: router_die, 9: router_end}
    def settle(side, at):
        d, k = at
        die(side, origin_of(side, d, 1 - core), at).wait_recv()
        die(side, origin_of(side, d, core), at).wait_send()

    def sent(side, at):
        d, k = at
        ring(side, origin_of(side, d - 1, core), at).wait_send()

    def settle_early():
        for k in range(K):
            die_own(partner, k).wait_recv()
            die_own(rows, k).wait_send()
        for side in range(2):
            raw_sent[side].wait_send()
            for at in ((0, 0),) + ARRIVALS[side][:SETTLED]:
                settle(side, at)
            for at in ARRIVALS[side]:
                if at[0] < 2:
                    sent(side, at)
        for copy in mx_sent + red_sent + r1 + [swap, share, meet]:
            copy.wait_send()

        @pl.when(first_core)
        def _():
            r1_die.wait_send()

        @pl.when(second_core)
        def _():
            for copy in rx + ry + [rd]:
                copy.wait_send()

    for j in range(STEPS):
        if j in between:
            between[j]()
        if j == STEPS - 2:
            settle_early()
        arrive(j)

    for side in range(2):
        for at in ARRIVALS[side][SETTLED:]:
            settle(side, at)
        for at in ARRIVALS[side]:
            if at[0] >= 2:
                sent(side, at)


PARTS = 2


def write(a, b, c, a_out, b_out, c_out, sems):
    tall = ROWS // PARTS
    copies = [
        pltpu.make_async_copy(a.at[e, pl.ds(i * tall, tall)], a_out.at[e, pl.ds(i * tall, tall)], sems.at[e * PARTS + i])
        for e in range(E) for i in range(PARTS)
    ]
    copies.append(pltpu.make_async_copy(b, b_out, sems.at[E * PARTS]))
    copies.append(pltpu.make_async_copy(c, c_out, sems.at[E * PARTS + 1]))
    for copy in copies:
        copy.start()
    for copy in copies:
        copy.wait()


def on_device(w_down, router_weight, router_gain):
    dma = pltpu.SemaphoreType.DMA
    shapes = (
        jax.ShapeDtypeStruct((E, ROWS, NR * LANES), BF16),
        jax.ShapeDtypeStruct((E, ROWS), F32),
        jax.ShapeDtypeStruct((E * X * Y, NR * LANES), BF16),
    )
    args = (w_down, router_weight.T, router_gain[None, :])
    held = pl.pallas_call(
        kernel,
        name="serve",
        out_shape=shapes,
        in_specs=[pl.BlockSpec(memory_space=pltpu.HBM)] * 3,
        out_specs=(pl.BlockSpec(memory_space=pltpu.VMEM),) * 3,
        scratch_shapes=[
            pltpu.VMEM((E, ROWS, LANES), F32),
            pltpu.VMEM((2, LANES), F32),
            pltpu.VMEM((1, LANES), F32),
            pltpu.VMEM((Z, BLOCKS, LANES), F32),
            pltpu.VMEM((BLOCKS, LANES), F32),
            pltpu.VMEM((2, BLOCKS, LANES), F32),
            pltpu.VMEM((2, HALF, LANES), F32),
            pltpu.VMEM((HALF, LANES), F32),
            pltpu.VMEM((Z, HALF, LANES), F32),
            pltpu.VMEM((2, HALF, LANES), F32),
            pltpu.VMEM((2, RAW, LANES), F32),
            pltpu.VMEM((2, LANES), BF16),
            pltpu.VMEM((X * Y, NR, 2, LANES), BF16),
            dma((4,)), pltpu.SemaphoreType.REGULAR, dma((Z,)), dma((Z + 1,)), dma(()), dma(()),
            dma(()), dma(()), dma((Z - 1,)), dma((Z,)), dma(()), dma(()),
            dma((2,)), dma((2,)), dma((2, 4 * K)), dma((4 * K,)), dma((4 * K,)),
            dma((2, 4 * K)), dma((2, 4 * K)), dma((K,)), dma((K,)),
            dma((Z,)), dma((NR,)), dma((X - 1,)), dma((X,)), dma((Y - 1,)), dma((Y,)), dma(()), dma(()),
        ],
        compiler_params=pltpu.CompilerParams(
            collective_id=0, has_side_effects=True, vmem_limit_bytes=24 * 1024 * 1024
        ),
    )(*(pltpu.with_memory_space_constraint(a, pltpu.HBM) for a in args))
    out, scale, router = pl.pallas_call(
        write,
        name="write",
        out_shape=shapes,
        in_specs=[pl.BlockSpec(memory_space=pltpu.VMEM)] * 3,
        out_specs=(pl.BlockSpec(memory_space=pltpu.HBM),) * 3,
        scratch_shapes=[dma((E * PARTS + 2,))],
        compiler_params=pltpu.CompilerParams(vmem_limit_bytes=24 * 1024 * 1024),
    )(*held)
    return out, scale, router.T


def solution(mesh):
    placed = (P("owner", None, "rows"), P("rows", "owner"), P("rows"))
    return jax.shard_map(
        on_device,
        mesh=mesh,
        in_specs=placed,
        out_specs=(P("owner", None, None), P("owner", None), P()),
        check_vma=False,
    )
```
